8 devices in a mesh: dp: 1 (over z), ep: 8 (over x, y, core).
Axes of the slice: x: 2, y: 2, z: 1, core: 2. Of those that a mesh axis runs over, the one named last changes fastest.
Arguments:
- x: bfloat16 [1, 8, 256, 3072], P('dp', 'ep')
- expert: int32 [1, 8, 256, 4], P('dp', 'ep')
- slot: int32 [1, 8, 256, 4], P('dp', 'ep')
- gate: float32 [1, 8, 256, 4], P('dp', 'ep')
- w_gate: bfloat16 [16, 3072, 10752], P('ep')
- w_up: bfloat16 [16, 3072, 10752], P('ep')
- w_down: bfloat16 [16, 10752, 3072], P('ep')
Outputs:
- y: bfloat16 [1, 8, 256, 3072], P('dp', 'ep')
All inputs are finite; a program needn't handle non-finite values.
Results may differ from the reference program's by a relative error of at most 0.009.
Values are sent between devices in bfloat16 or wider.
A program may use at most 2 GiB of HBM per device.

```python
import jax
import jax.numpy as jnp

MEMBERS = 8
TOKENS = 256
D = 3072
FF = 10752
TOP = 4
EXPERTS = 16
SLOTS = 5 * TOKENS * TOP // (4 * EXPERTS)


def setup_inputs(seed: int = 0, part: int = 0) -> dict:
    own, k1, k2, k3, k4, k5, k6 = jax.random.split(jax.random.key(seed), 7)
    kx, ke, kl, kg = jax.random.split(jax.random.fold_in(own, part), 4)
    devices = (1, MEMBERS)
    place = jax.random.permutation(kl, jnp.arange(EXPERTS, dtype=jnp.uint32))
    slow = ((EXPERTS + (9 * place) % EXPERTS) << ((9 * place) // EXPERTS)) // EXPERTS
    wait = (jax.random.bits(ke, (*devices, TOKENS, EXPERTS), jnp.uint32) >> 10) * slow
    expert = jnp.argsort(wait, axis=-1)[..., :TOP].astype(jnp.int32)
    chosen = jax.nn.one_hot(expert, EXPERTS, dtype=jnp.int32)
    in_line = jnp.cumsum(chosen.reshape(*devices, TOKENS * TOP, EXPERTS), axis=2) - 1
    slot = jnp.sum(in_line.reshape(chosen.shape) * chosen, axis=-1)

    def one(key, rows, columns):
        return (jax.random.normal(key, (rows, columns), jnp.float32) * rows**-0.5).astype(jnp.bfloat16)

    def weights(key, rows, columns):
        return jax.lax.map(lambda k: one(k, rows, columns), jax.random.split(key, EXPERTS))

    return {
        "x": jax.random.normal(kx, (*devices, TOKENS, D), jnp.float32).astype(jnp.bfloat16),
        "expert": expert,
        "slot": slot,
        "gate": jax.nn.softmax(jax.random.normal(kg, expert.shape, jnp.float32)),
        "w_gate": weights(k1, D, FF),
        "w_up": weights(k2, D, FF),
        "w_down": weights(k3, FF, D),
    }


def einsum(form, a, b):
    return jnp.einsum(form, a.astype(jnp.float32), b.astype(jnp.float32))


def reference(x, expert, slot, gate, w_gate, w_up, w_down):
    to_expert = jax.nn.one_hot(expert, EXPERTS, dtype=jnp.bfloat16)
    to_slot = jax.nn.one_hot(slot, SLOTS, dtype=jnp.bfloat16)
    weighted = to_expert * gate[..., None].astype(jnp.bfloat16)
    dispatch = einsum("abtke,abtkc->abtec", to_expert, to_slot).astype(jnp.bfloat16)
    combine = einsum("abtke,abtkc->abtec", weighted, to_slot).astype(jnp.bfloat16)
    z = einsum("abtec,abtd->aebcd", dispatch, x).astype(jnp.bfloat16)
    h = jax.nn.silu(einsum("aebcd,edf->aebcf", z, w_gate))
    h = (h * einsum("aebcd,edf->aebcf", z, w_up)).astype(jnp.bfloat16)
    out = einsum("aebcf,efd->aebcd", h, w_down).astype(jnp.bfloat16)
    y = einsum("abtec,aebcd->abtd", combine, out)
    return y.astype(jnp.bfloat16)
```

```python
import functools

import jax
import jax.numpy as jnp
from jax import lax
from jax.experimental import pallas as pl
from jax.experimental.pallas import tpu as pltpu
from jax.sharding import PartitionSpec as P

CHUNK = 16
ROWS = (256, 384, 512, 640)
TF = 512
TK = 1536
COLS = (768, 768, 768, 768)


def by_rows(total, rows, f):
    low = 0
    for m in rows:
        high = m // CHUNK
        pl.when((total > low) & (total <= high))(functools.partial(f, m))
        low = high


def up_kernel(slots, n_ref, off_ref, tot_ref, z_hbm, wg_ref, wu_ref, h_ref, z_ref, sem):
    e, j = pl.program_id(0), pl.program_id(1)
    devices = z_hbm.shape[0]

    def piece(k, s, q):
        row = pl.multiple_of(k * slots + q * CHUNK, CHUNK)
        to = pl.multiple_of((off_ref[k, s] + q) * CHUNK, CHUNK)
        return pltpu.make_async_copy(
            z_hbm.at[s, pl.ds(row, CHUNK), :], z_ref.at[k, pl.ds(to, CHUNK), :], sem.at[k]
        )

    @pl.when((e == 0) & (j == 0))
    def _():
        for k in range(2):
            for s in range(devices):
                @pl.loop(0, n_ref[k, s])
                def _(q):
                    piece(k, s, q).start()

            @pl.loop(tot_ref[k], z_ref.shape[1] // CHUNK)
            def _(q):
                to = pl.multiple_of(q * CHUNK, CHUNK)
                z_ref[k, pl.ds(to, CHUNK), :] = jnp.zeros((CHUNK, z_ref.shape[2]), z_ref.dtype)

    @pl.when(j == 0)
    def _():
        @pl.loop(0, tot_ref[e])
        def _(q):
            piece(e, 0, 0).wait()

    def compute(m):
        z = z_ref[e, :m, :]
        g = jnp.dot(z, wg_ref[0], preferred_element_type=jnp.float32)
        u = jnp.dot(z, wu_ref[0], preferred_element_type=jnp.float32)
        h_ref[0, :m, :] = (jax.nn.silu(g) * u).astype(h_ref.dtype)

    by_rows(tot_ref[e], ROWS, compute)


def down_kernel(slots, n_ref, off_ref, tot_ref, h_ref, w_ref, out_hbm, acc_ref, o_ref, zero_ref, sem):
    e, k = pl.program_id(0), pl.program_id(1)
    devices = out_hbm.shape[0]
    last = pl.num_programs(1) - 1
    per = slots // CHUNK

    @pl.when((e == 0) & (k == 0))
    def _():
        zero_ref[...] = jnp.zeros_like(zero_ref)

    def compute(m):
        part = jnp.dot(h_ref[0, :m, :], w_ref[0], preferred_element_type=jnp.float32)

        @pl.when(k == 0)
        def _():
            acc_ref[:m, :] = part

        @pl.when(k > 0)
        def _():
            acc_ref[:m, :] += part

    by_rows(tot_ref[e], ROWS, compute)

    def put(src, s, q):
        row = pl.multiple_of(e * slots + q * CHUNK, CHUNK)
        return pltpu.make_async_copy(src, out_hbm.at[s, pl.ds(row, CHUNK), :], sem)

    @pl.when(k == last)
    def _():
        o_ref[e] = acc_ref[...].astype(o_ref.dtype)
        for s in range(devices):
            @pl.loop(0, n_ref[e, s])
            def _(q):
                at = pl.multiple_of((off_ref[e, s] + q) * CHUNK, CHUNK)
                put(o_ref.at[e, pl.ds(at, CHUNK), :], s, q).start()

            @pl.loop(n_ref[e, s], per)
            def _(q):
                put(zero_ref, s, q).start()

        @pl.when(e == 1)
        def _():
            @pl.loop(0, 2 * devices * per)
            def _(q):
                put(zero_ref, 0, 0).wait()


def solution(mesh):
    devices = mesh.shape["ep"]

    def up(counts, z, w_gate, w_up, slots):
        held, d, ff = w_gate.shape
        rows = devices * slots
        return pl.pallas_call(
            functools.partial(up_kernel, slots),
            out_shape=jax.ShapeDtypeStruct((held, rows, ff), jnp.bfloat16),
            grid_spec=pltpu.PrefetchScalarGridSpec(
                num_scalar_prefetch=3,
                grid=(held, ff // TF),
                in_specs=[
                    pl.BlockSpec(memory_space=pl.ANY),
                    pl.BlockSpec((1, d, TF), lambda e, j, *_: (e, 0, j)),
                    pl.BlockSpec((1, d, TF), lambda e, j, *_: (e, 0, j)),
                ],
                out_specs=pl.BlockSpec((1, rows, TF), lambda e, j, *_: (e, 0, j)),
                scratch_shapes=[
                    pltpu.VMEM((held, rows, d), jnp.bfloat16),
                    pltpu.SemaphoreType.DMA((held,)),
                ],
            ),
            cost_estimate=pl.CostEstimate(
                flops=4 * held * rows * d * ff, bytes_accessed=4 * held * d * ff, transcendentals=0
            ),
            name="up",
        )(*counts, z, w_gate, w_up)

    def down(counts, h, w_down, slots, first, width):
        held, ff, d = w_down.shape
        rows = devices * slots
        at = first // width
        return pl.pallas_call(
            functools.partial(down_kernel, slots),
            out_shape=jax.ShapeDtypeStruct((devices, held * slots, width), jnp.bfloat16),
            grid_spec=pltpu.PrefetchScalarGridSpec(
                num_scalar_prefetch=3,
                grid=(held, ff // TK),
                in_specs=[
                    pl.BlockSpec((1, rows, TK), lambda e, k, *_: (e, 0, k)),
                    pl.BlockSpec((1, TK, width), lambda e, k, *_: (e, k, at)),
                ],
                out_specs=pl.BlockSpec(memory_space=pl.ANY),
                scratch_shapes=[
                    pltpu.VMEM((rows, width), jnp.float32),
                    pltpu.VMEM((held, rows, width), jnp.bfloat16),
                    pltpu.VMEM((CHUNK, width), jnp.bfloat16),
                    pltpu.SemaphoreType.DMA,
                ],
            ),
            cost_estimate=pl.CostEstimate(
                flops=2 * held * rows * width * ff, bytes_accessed=2 * held * width * ff, transcendentals=0
            ),
            name="down",
        )(*counts, h, w_down)

    def body(x, expert, slot, gate, w_gate, w_up, w_down):
        x, expert, slot, gate = x[0, 0], expert[0, 0], slot[0, 0], gate[0, 0]
        tokens, top = expert.shape
        held, d, ff = w_gate.shape
        experts = held * devices
        slots = 5 * tokens * top // (4 * experts)
        pos = jnp.where(slot < slots, expert * slots + slot, -1)
        weight = gate.astype(jnp.bfloat16).astype(jnp.float32)
        note = jnp.concatenate([pos.astype(jnp.float32), weight], axis=1)
        note = lax.all_gather(note, "ep")
        xs = lax.all_gather(x, "ep")
        here = held * slots
        pos = note[..., :top].astype(jnp.int32) - lax.axis_index("ep") * here
        weight = note[..., top:]
        hit = pos[..., None, :] == jnp.arange(here)[:, None]
        pick = jnp.any(hit, axis=-1).astype(jnp.bfloat16)
        combine = jnp.sum(jnp.where(hit, weight[..., None, :], 0.0), axis=-1).astype(jnp.bfloat16)
        ends = jnp.stack(
            [
                jnp.max(jnp.where((pos >= k * slots) & (pos < (k + 1) * slots), pos - k * slots + 1, 0), axis=(1, 2))
                for k in range(held)
            ]
        )
        n = (ends + CHUNK - 1) // CHUNK
        off = jnp.cumsum(n, axis=1) - n
        counts = (n, off, jnp.sum(n, axis=1))
        z = jnp.einsum("stc,std->scd", pick, xs, preferred_element_type=jnp.float32).astype(jnp.bfloat16)
        h = up(counts, z, w_gate, w_up, slots)
        first, parts = 0, []
        for width in COLS:
            out = down(counts, h, w_down, slots, first, width)
            part = jnp.einsum("stc,scd->std", combine, out, preferred_element_type=jnp.float32).astype(jnp.bfloat16)
            parts.append(lax.psum_scatter(part, "ep", scatter_dimension=0))
            first += width
        return jnp.concatenate(parts, axis=-1)[None, None]

    held = P("ep", None, None)
    own = P("dp", "ep", None, None)
    return jax.shard_map(
        body,
        mesh=mesh,
        in_specs=(own, own, own, own, held, held, held),
        out_specs=own,
        check_vma=False,
    )
```
